32 devices in a mesh: row: 8 (over z, x), col: 4 (over y, core).
Axes of the slice: x: 2, y: 2, z: 4, core: 2. Of those that a mesh axis runs over, the one named last changes fastest.
Arguments:
- embedding: float32 [8192, 128], P(('row', 'col')), may hold values from -6 to 6
- degrees: int32 [8192], P(('row', 'col')), may hold values from 16 to 64
- tile_values: bfloat16 [8, 4, 128, 256, 256], P('row', 'col'), may hold values from -0.1796875 to 0.1796875
- tile_layout: int32 [8, 4, 128, 2], P('row', 'col'), may hold values from 0 to 7, as said below
- tile_count: int32 [8, 4], P('row', 'col'), may hold values from 16 to 128, as said below
- coefficients: float32 [7], replicated, may hold values from -1 to 1
Outputs:
- filtered: float32 [8192, 128], P(('row', 'col'))
The draws below stay inside these ranges and needn't reach their ends.
Inputs may be any that keep to these rules, and one draw needn't show every extreme that they name: `tile_layout`: entry [r, c, s, 0] is a row block below 8 and entry [r, c, s, 1] a column block below 4; entries of slots at or past tile_count[r, c] are valid but unused; a place may repeat. `tile_count`: some device has all 128 slots live.
All inputs are finite; a program needn't handle non-finite values.
Results may differ from the reference program's by a relative error of at most 0.0015.
Values may be sent and summed in bfloat16 or wider, within the bound.
A program may use at most 128 MiB of HBM per device.

```python
import jax
import jax.numpy as jnp
from jax import lax

F = 128
BLOCK = 256
BLOCKS_DEV = 1
SLOTS = 128
ORDER = 6
PIECE = 256
ROW_BLOCKS = 8
COL_BLOCKS = 4
NODES = 8192
N_ROW = 8
N_COL = 4


def draw_tile_count(key, part):
    key_base = jax.random.fold_in(key, 11)
    key_heavy = jax.random.fold_in(key, 12)
    key_pick = jax.random.fold_in(key, 13)
    key_full = jax.random.fold_in(key, 14)
    lowest = max(1, SLOTS // 8)
    base = jax.random.randint(key_base, (N_ROW * N_COL,), lowest, SLOTS // 2 + 1)
    heavy = jax.random.randint(key_heavy, (N_ROW * N_COL,), SLOTS // 2, SLOTS + 1)
    pick = jax.random.randint(key_pick, (N_ROW * N_COL,), 0, 8)
    counts = jnp.where(pick == 0, heavy, base)
    full_device = jax.random.randint(key_full, (), 0, N_ROW * N_COL)
    counts = jnp.where(jnp.arange(N_ROW * N_COL) == full_device, SLOTS, counts)
    return counts.reshape(N_ROW, N_COL).astype(jnp.int32)


def draw_tile_layout(key, part):
    key_rows = jax.random.fold_in(key, 21)
    key_hub = jax.random.fold_in(key, 22)
    key_pick = jax.random.fold_in(key, 23)
    key_cols = jax.random.fold_in(key, 24)
    rows_any = jax.random.randint(key_rows, (N_ROW, N_COL, SLOTS), 0, ROW_BLOCKS)
    hub_rows = jax.random.randint(key_hub, (N_ROW, N_COL, 1), 0, ROW_BLOCKS)
    pick = jax.random.randint(key_pick, (N_ROW, N_COL, SLOTS), 0, 2)
    rows_all = jnp.where(pick == 1, hub_rows, rows_any)
    cols_all = jax.random.randint(key_cols, (N_ROW, N_COL, SLOTS), 0, COL_BLOCKS)
    return jnp.stack([rows_all, cols_all], axis=-1).astype(jnp.int32)


def touch_ends(drawn, own_key, least, largest):
    place = [jax.random.randint(jax.random.fold_in(own_key, axis), (), 0, length) for axis, length in enumerate(drawn.shape)]
    longest = drawn.shape.index(max(drawn.shape))
    beside = place[:longest] + [(place[longest] + 1) % drawn.shape[longest]] + place[longest + 1:]
    return drawn.at[tuple(place)].set(least).at[tuple(beside)].set(largest)


def shard_levels(rng, shape, pieces, smallest, high):
    loudness, own = 1.0, jax.random.fold_in(rng, 6)
    for axis_at, parts in pieces:
        steps = jnp.exp(jax.random.uniform(jax.random.fold_in(own, axis_at), (parts,), jnp.float32, smallest / len(pieces), high / len(pieces)))
        loudness = loudness * jnp.repeat(steps, shape[axis_at] // parts).reshape([-1 if axis == axis_at else 1 for axis in range(len(shape))])
    return loudness


def normal_values(key, extent, width, limit, pieces=(), held_as=jnp.bfloat16):
    values = jax.random.normal(key, extent, jnp.float32) * width
    if len(pieces) > 0:
        values = shard_levels(key, extent, pieces, -0.22, 0.18) * values
    return jnp.clip(values, min=-limit, max=limit).astype(held_as)


def setup_inputs(seed: int = 0) -> dict:
    seeds = jax.random.split(jax.random.key(seed), 7)
    return {
        "embedding": normal_values(seeds[0], (NODES, F), 1.0, 6.0, ((0, 32),), jnp.float32),
        "degrees": touch_ends(jax.random.randint(seeds[1], (NODES,), 16, 65), jax.random.fold_in(seeds[1], 1), 16, 64).astype(jnp.int32),
        "tile_values": normal_values(seeds[2], (N_ROW, N_COL, SLOTS, BLOCK, BLOCK), 0.03, 0.1796875, ((0, 8), (1, 4))),
        "tile_layout": draw_tile_layout(jax.random.fold_in(seeds[6], 71), 0),
        "tile_count": draw_tile_count(jax.random.fold_in(seeds[6], 71), 0),
        "coefficients": jnp.clip(jax.random.uniform(seeds[5], (ORDER + 1,), jnp.float32, -1.0, 1.0), -1.0, 1.0),
    }


spectral_shift = 0.5

def reference(embedding, degrees, tile_values, tile_layout, tile_count, coefficients):
    inv_root = lax.rsqrt(degrees.astype(jnp.float32))[:, None]

    def operate(vector):
        scaled = (inv_root * vector).astype(jnp.bfloat16)

        def device_step(device_num, running):
            row_group = device_num // N_COL
            col_group = device_num % N_COL
            live_count = tile_count[row_group, col_group]

            def slot_step(slot_num, inner):
                row_block = tile_layout[row_group, col_group, slot_num, 0]
                col_block = tile_layout[row_group, col_group, slot_num, 1]
                col_start = ((row_group * COL_BLOCKS + col_block) * BLOCK).astype(jnp.int32)
                row_start = ((row_block // BLOCKS_DEV * N_COL + col_group) * PIECE + row_block % BLOCKS_DEV * BLOCK).astype(jnp.int32)
                source = lax.dynamic_slice_in_dim(scaled, col_start, BLOCK, 0)
                product = jnp.dot(tile_values[row_group, col_group, slot_num], source, preferred_element_type=jnp.float32)
                before = lax.dynamic_slice_in_dim(inner, row_start, BLOCK, 0)
                return lax.dynamic_update_slice_in_dim(inner, before + product, row_start, 0)
            return lax.fori_loop(jnp.int32(0), live_count, slot_step, running)
        summed = lax.fori_loop(0, N_ROW * N_COL, device_step, jnp.zeros(vector.shape, jnp.float32))
        return (1.0 - spectral_shift) * vector - inv_root * summed
    previous = embedding
    current = operate(embedding)
    filtered = coefficients[0] * previous + coefficients[1] * current
    for order in range(2, ORDER + 1):
        following = 2.0 * operate(current) - previous
        filtered = filtered + coefficients[order] * following
        previous, current = (current, following)
    return filtered
```

```python
import functools

import jax
import jax.numpy as jnp
from jax import lax
from jax.experimental import pallas as pl
from jax.experimental.pallas import tpu as pltpu
from jax.sharding import PartitionSpec as P

ORDER = 6
SHIFT = 0.5
CHUNK = 4
DEPTH = 8
MESH = pl.DeviceIdType.MESH
VMEM_LIMIT = 60 * 1024 * 1024


def merge_kernel(n_row, n_col, count_ref, layout_ref, tiles_ref, hi_ref, lo_ref,
                 total, landed, stage, in_sem, out_sem):
    block = tiles_ref.shape[1]
    count = count_ref[0]
    chunks = (count + CHUNK - 1) // CHUNK

    def fetch(chunk):
        slot = lax.rem(chunk, DEPTH)
        return pltpu.make_async_copy(
            tiles_ref.at[pl.ds(chunk * CHUNK, CHUNK)], landed.at[slot], in_sem.at[slot])

    for ahead in range(DEPTH):
        @pl.when(ahead < chunks)
        def _():
            fetch(jnp.int32(ahead)).start()

    def clear(place, carry):
        total[place] = jnp.zeros((block, block), jnp.float32)
        return carry

    lax.fori_loop(0, n_row * n_col, clear, 0)

    def add_chunk(chunk, carry):
        slot = lax.rem(chunk, DEPTH)
        fetch(chunk).wait()
        for inner in range(CHUNK):
            number = chunk * CHUNK + inner

            @pl.when(number < count)
            def _():
                place = layout_ref[2 * number] * n_col + layout_ref[2 * number + 1]
                total[place] += landed[slot, inner].astype(jnp.float32)

        @pl.when(chunk + DEPTH < chunks)
        def _():
            fetch(chunk + DEPTH).start()
        return carry

    lax.fori_loop(0, chunks, add_chunk, 0)

    def outgoing(row):
        slot = lax.rem(row, 2)
        return (pltpu.make_async_copy(stage.at[slot, 0], hi_ref.at[row], out_sem.at[slot, 0]),
                pltpu.make_async_copy(stage.at[slot, 1], lo_ref.at[row], out_sem.at[slot, 1]))

    def put_row(row, carry):
        slot = lax.rem(row, 2)

        @pl.when(row >= 2)
        def _():
            for copy in outgoing(row - 2):
                copy.wait()
        for col in range(n_col):
            value = total[row * n_col + col]
            high = value.astype(jnp.bfloat16)
            stage[slot, 0, :, col * block:(col + 1) * block] = high
            stage[slot, 1, :, col * block:(col + 1) * block] = (
                value - high.astype(jnp.float32)).astype(jnp.bfloat16)
        for copy in outgoing(row):
            copy.start()
        return carry

    lax.fori_loop(0, n_row, put_row, 0)
    for row in (n_row - 2, n_row - 1):
        for copy in outgoing(jnp.int32(row)):
            copy.wait()


def filter_kernel(nz, nx, nc, coef_ref, emb_ref, inv_ref, hi_ref, lo_ref, out_ref,
                  prev, cur, field, part_a, part_b, rx_a, rx_b, zr_a, zr_b,
                  ag_send, ag_recv, xa_send, xa_recv, za_send, za_recv,
                  zb_send, zb_recv, xb_send, xb_recv):
    r = lax.axis_index("row")
    c = lax.axis_index("col")
    z, x = r // nx, lax.rem(r, nx)
    piece = emb_ref.shape[0]
    half = piece // 2

    def rows_of(owner, part):
        return pl.ds(pl.multiple_of(owner * piece + part * half, half), half)

    def remote(src, dst, send_sem, recv_sem, **where):
        return pltpu.make_async_remote_copy(
            src_ref=src, dst_ref=dst, send_sem=send_sem, recv_sem=recv_sem,
            device_id={"row": where.get("row", r), "col": where.get("col", c)},
            device_id_type=MESH)

    def gather_copy(p, part, offset, owner):
        spot = field.at[p, rows_of(owner, part)]
        return remote(spot, spot, ag_send.at[part, offset], ag_recv.at[p, part, owner],
                      col=lax.rem(c + offset, nc))

    def cross_a(p, d, other, source):
        return remote(part_a.at[d, other], rx_a.at[p, d, source],
                      xa_send.at[d, other], xa_recv.at[p, d, source], row=z * nx + other)

    def cross_b(p, other, source):
        return remote(part_b.at[z, other], rx_b.at[p, source],
                      xb_send.at[other], xb_recv.at[p, source], row=z * nx + other)

    def line_a(p, way, d, neighbour):
        return remote(part_a.at[d, x], zr_a.at[p, way, d],
                      za_send.at[d], za_recv.at[p, way, d], row=neighbour * nx + x)

    def line_b(p, way, d, neighbour):
        return remote(part_b.at[d], zr_b.at[p, way, d],
                      zb_send.at[d], zb_recv.at[p, way, d], row=neighbour * nx + x)

    def visit(t):
        d = jnp.where(2 * z >= nz, t, nz - 1 - t)
        upward = d > z
        way = jnp.where(upward, 0, 1)
        neighbour = jnp.clip(jnp.where(upward, z + 1, z - 1), 0, nz - 1)
        first = jnp.where(upward, z == 0, z == nz - 1)
        return d, way, neighbour, first

    others = [lax.rem(x + 1 + u, nx) for u in range(nx - 1)]

    def share(p, part, value):
        field[p, rows_of(c, part)] = value.astype(jnp.bfloat16)
        for offset in range(1, nc):
            gather_copy(p, part, offset, c).start()

    barrier = pltpu.get_barrier_semaphore()
    for other in others:
        pl.semaphore_signal(barrier, inc=1, device_id={"row": z * nx + other, "col": c},
                            device_id_type=MESH)
    for offset in range(1, nc):
        pl.semaphore_signal(barrier, inc=1, device_id={"row": r, "col": lax.rem(c + offset, nc)},
                            device_id_type=MESH)

    @pl.when(z > 0)
    def _():
        pl.semaphore_signal(barrier, inc=1, device_id={"row": r - nx, "col": c},
                            device_id_type=MESH)

    @pl.when(z < nz - 1)
    def _():
        pl.semaphore_signal(barrier, inc=1, device_id={"row": r + nx, "col": c},
                            device_id_type=MESH)
    pl.semaphore_wait(barrier, nx - 1 + nc - 1 + jnp.where(z > 0, 1, 0)
                      + jnp.where(z < nz - 1, 1, 0))

    start = emb_ref[...]
    prev[...] = start
    cur[...] = start
    out_ref[...] = coef_ref[0] * start
    for part in range(2):
        span = slice(part * half, (part + 1) * half)
        share(0, part, inv_ref[span] * emb_ref[span])

    def step(k, carry):
        p = lax.rem(k, 2)
        for offset in range(1, nc):
            for part in range(2):
                copy = gather_copy(p, part, offset, lax.rem(c + offset, nc))
                copy.wait_send()
                copy.wait_recv()

        def multiply(t, inner):
            d, way, neighbour, first = visit(t)
            for u in range(nx):
                other = lax.rem(x + 1 + u, nx)
                number = d * nx + other
                source = field[p]
                value = (jnp.dot(hi_ref[number], source, preferred_element_type=jnp.float32)
                         + jnp.dot(lo_ref[number], source, preferred_element_type=jnp.float32))
                part_a[d, other] = value[:half]
                part_b[d, other] = value[half:]
                if u < nx - 1:
                    cross_a(p, d, other, x).start()

            @pl.when((d != z) & first)
            def _():
                line_b(p, way, d, neighbour).start()
            return inner

        lax.fori_loop(0, nz, multiply, 0)

        def collect_a(d):
            for other in others:
                cross_a(p, d, other, other).wait_recv()
                part_a[d, x] += rx_a[p, d, other]

        def pass_on(t, inner):
            d, way, neighbour, first = visit(t)

            @pl.when((d != z) & jnp.logical_not(first))
            def _():
                line_b(p, way, d, neighbour).wait_recv()
                part_b[d] += zr_b[p, way, d]
                line_b(p, way, d, neighbour).start()

            @pl.when(d != z)
            def _():
                collect_a(d)

                @pl.when(jnp.logical_not(first))
                def _():
                    line_a(p, way, d, neighbour).wait_recv()
                    part_a[d, x] += zr_a[p, way, d]
                line_a(p, way, d, neighbour).start()
            return inner

        lax.fori_loop(0, nz, pass_on, 0)

        arrivals = ((0, z > 0), (1, z < nz - 1))
        for way, there in arrivals:
            @pl.when(there)
            def _():
                line_b(p, way, z, z).wait_recv()
                part_b[z] += zr_b[p, way, z]
        for other in others:
            cross_b(p, other, x).start()
        collect_a(z)
        for way, there in arrivals:
            @pl.when(there)
            def _():
                line_a(p, way, z, z).wait_recv()
                part_a[z, x] += zr_a[p, way, z]

        alpha = jnp.where(k == 0, 1.0, 2.0).astype(jnp.float32)
        beta = jnp.where(k == 0, 0.0, 1.0).astype(jnp.float32)
        weight = coef_ref[k + 1]

        def finish(part, summed):
            span = slice(part * half, (part + 1) * half)
            now = cur[span]
            moved = (1.0 - SHIFT) * now - inv_ref[span] * summed
            following = alpha * moved - beta * prev[span]
            prev[span] = now
            cur[span] = following
            out_ref[span] = out_ref[span] + weight * following

            @pl.when(k < ORDER - 1)
            def _():
                share(1 - p, part, inv_ref[span] * following)

        finish(0, part_a[z, x])
        summed = part_b[z, x]
        for other in others:
            cross_b(p, other, other).wait_recv()
            summed = summed + rx_b[p, other]
        finish(1, summed)

        for other in others:
            cross_b(p, other, x).wait_send()

        def drain(t, inner):
            d, way, neighbour, first = visit(t)
            for other in others:
                cross_a(p, d, other, x).wait_send()

            @pl.when(d != z)
            def _():
                line_a(p, way, d, neighbour).wait_send()
                line_b(p, way, d, neighbour).wait_send()
            return inner

        lax.fori_loop(0, nz, drain, 0)
        return carry

    lax.fori_loop(0, ORDER, step, 0)


def grid_of(n):
    nx = 1
    while nx * nx * 4 <= n and n % (nx * 2) == 0:
        nx *= 2
    return n // nx, nx


def solution(mesh):
    n_row, n_col = mesh.shape["row"], mesh.shape["col"]
    nz, nx = grid_of(n_row)

    def per_device(embedding, degrees, tile_values, tile_layout, tile_count, coefficients):
        tiles = tile_values[0, 0]
        block = tiles.shape[1]
        piece, width = embedding.shape
        half = piece // 2
        inv = lax.rsqrt(degrees.astype(jnp.float32))[:, None]
        inv = jnp.broadcast_to(inv, (piece, width))
        smem = pl.BlockSpec(memory_space=pltpu.SMEM)
        vmem = pl.BlockSpec(memory_space=pltpu.VMEM)
        anywhere = pl.BlockSpec(memory_space=pl.ANY)
        weight = jax.ShapeDtypeStruct((n_row, block, n_col * block), jnp.bfloat16)
        high, low = pl.pallas_call(
            functools.partial(merge_kernel, n_row, n_col),
            out_shape=(weight, weight),
            in_specs=[smem, smem, anywhere],
            out_specs=(anywhere, anywhere),
            scratch_shapes=[
                pltpu.VMEM((n_row * n_col, block, block), jnp.float32),
                pltpu.VMEM((DEPTH, CHUNK, block, block), jnp.bfloat16),
                pltpu.VMEM((2, 2, block, n_col * block), jnp.bfloat16),
                pltpu.SemaphoreType.DMA((DEPTH,)),
                pltpu.SemaphoreType.DMA((2, 2)),
            ],
            compiler_params=pltpu.CompilerParams(vmem_limit_bytes=VMEM_LIMIT),
        )(tile_count.reshape(1), tile_layout.reshape(-1), tiles)
        dma = pltpu.SemaphoreType.DMA
        f32 = jnp.float32
        return pl.pallas_call(
            functools.partial(filter_kernel, nz, nx, n_col),
            out_shape=jax.ShapeDtypeStruct((piece, width), f32),
            in_specs=[smem, vmem, vmem, vmem, vmem],
            out_specs=vmem,
            scratch_shapes=[
                pltpu.VMEM((piece, width), f32),
                pltpu.VMEM((piece, width), f32),
                pltpu.VMEM((2, n_col * piece, width), jnp.bfloat16),
                pltpu.VMEM((nz, nx, half, width), f32),
                pltpu.VMEM((nz, nx, half, width), f32),
                pltpu.VMEM((2, nz, nx, half, width), f32),
                pltpu.VMEM((2, nx, half, width), f32),
                pltpu.VMEM((2, 2, nz, half, width), f32),
                pltpu.VMEM((2, 2, nz, nx, half, width), f32),
                dma((2, n_col)), dma((2, 2, n_col)),
                dma((nz, nx)), dma((2, nz, nx)),
                dma((nz,)), dma((2, 2, nz)),
                dma((nz,)), dma((2, 2, nz)),
                dma((nx,)), dma((2, nx)),
            ],
            compiler_params=pltpu.CompilerParams(
                collective_id=0, has_side_effects=True, vmem_limit_bytes=VMEM_LIMIT),
        )(coefficients, embedding, inv, high, low)

    return jax.shard_map(
        per_device, mesh=mesh,
        in_specs=(P(("row", "col"), None), P(("row", "col")),
                  P("row", "col", None, None, None), P("row", "col", None, None),
                  P("row", "col"), P()),
        out_specs=P(("row", "col"), None), check_vma=False)
```

```python
import functools

import jax
import jax.numpy as jnp
from jax import lax
from jax.experimental import pallas as pl
from jax.experimental.pallas import tpu as pltpu
from jax.sharding import PartitionSpec as P

ORDER = 6
SHIFT = 0.5
CHUNK = 4
DEPTH = 8
PIECES = 2
MESH = pl.DeviceIdType.MESH
VMEM_LIMIT = 60 * 1024 * 1024


def merge_kernel(n_row, n_col, count_ref, layout_ref, tiles_ref, hi_ref, lo_ref,
                 total, landed, stage, in_sem, out_sem):
    block = tiles_ref.shape[1]
    count = count_ref[0]
    chunks = (count + CHUNK - 1) // CHUNK

    def fetch(chunk):
        slot = lax.rem(chunk, DEPTH)
        return pltpu.make_async_copy(
            tiles_ref.at[pl.ds(chunk * CHUNK, CHUNK)], landed.at[slot], in_sem.at[slot])

    for ahead in range(DEPTH):
        @pl.when(ahead < chunks)
        def _():
            fetch(jnp.int32(ahead)).start()

    def clear(place, carry):
        total[place] = jnp.zeros((block, block), jnp.float32)
        return carry

    lax.fori_loop(0, n_row * n_col, clear, 0)

    def add_chunk(chunk, carry):
        slot = lax.rem(chunk, DEPTH)
        fetch(chunk).wait()
        for inner in range(CHUNK):
            number = chunk * CHUNK + inner

            @pl.when(number < count)
            def _():
                place = layout_ref[2 * number] * n_col + layout_ref[2 * number + 1]
                total[place] += landed[slot, inner].astype(jnp.float32)

        @pl.when(chunk + DEPTH < chunks)
        def _():
            fetch(chunk + DEPTH).start()
        return carry

    lax.fori_loop(0, chunks, add_chunk, 0)

    def outgoing(row):
        slot = lax.rem(row, 2)
        return (pltpu.make_async_copy(stage.at[slot, 0], hi_ref.at[row], out_sem.at[slot, 0]),
                pltpu.make_async_copy(stage.at[slot, 1], lo_ref.at[row], out_sem.at[slot, 1]))

    def put_row(row, carry):
        slot = lax.rem(row, 2)

        @pl.when(row >= 2)
        def _():
            for copy in outgoing(row - 2):
                copy.wait()
        for col in range(n_col):
            value = total[row * n_col + col]
            high = value.astype(jnp.bfloat16)
            stage[slot, 0, :, col * block:(col + 1) * block] = high
            stage[slot, 1, :, col * block:(col + 1) * block] = (
                value - high.astype(jnp.float32)).astype(jnp.bfloat16)
        for copy in outgoing(row):
            copy.start()
        return carry

    lax.fori_loop(0, n_row, put_row, 0)
    for row in (n_row - 2, n_row - 1):
        for copy in outgoing(jnp.int32(row)):
            copy.wait()


def filter_kernel(nz, nx, nc, coef_ref, emb_ref, inv_ref, hi_ref, lo_ref, out_ref,
                  weights, prev, cur, field, part_a, part_b, tx_a, tx_b, rx_a, rx_b, zr_a, zr_b,
                  w_sem, ag_send, ag_recv, xa_send, xa_recv, za_send, za_recv,
                  zb_send, zb_recv, xb_send, xb_recv):
    r = lax.axis_index("row")
    c = lax.axis_index("col")
    z, x = r // nx, lax.rem(r, nx)
    piece = emb_ref.shape[0]
    half = piece // 2
    quarter = half // PIECES

    def rows_of(owner, part):
        return pl.ds(pl.multiple_of(owner * piece + part * half, half), half)

    def remote(src, dst, send_sem, recv_sem, **where):
        return pltpu.make_async_remote_copy(
            src_ref=src, dst_ref=dst, send_sem=send_sem, recv_sem=recv_sem,
            device_id={"row": where.get("row", r), "col": where.get("col", c)},
            device_id_type=MESH)

    def gather_copy(p, part, offset, owner):
        spot = field.at[p, rows_of(owner, part)]
        return remote(spot, spot, ag_send.at[part, offset], ag_recv.at[p, part, owner],
                      col=lax.rem(c + offset, nc))

    def cross_a(p, d, other, source):
        return remote(tx_a.at[d, other], rx_a.at[p, d, source],
                      xa_send.at[d, other], xa_recv.at[p, d, source], row=z * nx + other)

    def cross_b(p, other, source):
        return remote(part_b.at[other], rx_b.at[p, source],
                      xb_send.at[other], xb_recv.at[p, source], row=z * nx + other)

    def line_a(p, way, d, q, neighbour):
        rows = pl.ds(q * quarter, quarter)
        return remote(part_a.at[d, rows], zr_a.at[p, way, d, rows],
                      za_send.at[d, q], za_recv.at[p, way, d, q], row=neighbour * nx + x)

    def line_b(p, d, source):
        return remote(tx_b.at[d], zr_b.at[p, source],
                      zb_send.at[d], zb_recv.at[p, source], row=d * nx + x)

    def weight_copies(number):
        return (pltpu.make_async_copy(hi_ref.at[number], weights.at[0, number], w_sem.at[0, number]),
                pltpu.make_async_copy(lo_ref.at[number], weights.at[1, number], w_sem.at[1, number]))

    def visit(t):
        d = jnp.where(2 * z >= nz, t, nz - 1 - t)
        upward = d > z
        way = jnp.where(upward, 0, 1)
        neighbour = jnp.clip(jnp.where(upward, z + 1, z - 1), 0, nz - 1)
        first = jnp.where(upward, z == 0, z == nz - 1)
        return d, way, neighbour, first

    others = [lax.rem(x + 1 + u, nx) for u in range(nx - 1)]
    levels = [lax.rem(z + 1 + u, nz) for u in range(nz - 1)]

    def share(p, part, value):
        field[p, rows_of(c, part)] = value.astype(jnp.bfloat16)
        for offset in range(1, nc):
            gather_copy(p, part, offset, c).start()

    def load(t, carry):
        d = visit(t)[0]
        for u in range(nx):
            for copy in weight_copies(d * nx + lax.rem(x + 1 + u, nx)):
                copy.start()
        return carry

    barrier = pltpu.get_barrier_semaphore()
    for other in others:
        pl.semaphore_signal(barrier, inc=1, device_id={"row": z * nx + other, "col": c},
                            device_id_type=MESH)
    for level in levels:
        pl.semaphore_signal(barrier, inc=1, device_id={"row": level * nx + x, "col": c},
                            device_id_type=MESH)
    for offset in range(1, nc):
        pl.semaphore_signal(barrier, inc=1, device_id={"row": r, "col": lax.rem(c + offset, nc)},
                            device_id_type=MESH)
    lax.fori_loop(0, nz, load, 0)
    start = emb_ref[...]
    prev[...] = start
    cur[...] = start
    out_ref[...] = coef_ref[0] * start
    pl.semaphore_wait(barrier, nx - 1 + nz - 1 + nc - 1)
    for part in range(2):
        span = slice(part * half, (part + 1) * half)
        share(0, part, inv_ref[span] * emb_ref[span])

    def step(k, carry):
        p = lax.rem(k, 2)
        for offset in range(1, nc):
            for part in range(2):
                copy = gather_copy(p, part, offset, lax.rem(c + offset, nc))
                copy.wait_send()
                copy.wait_recv()

        def multiply(t, inner):
            d = visit(t)[0]
            for u in range(nx):
                other = lax.rem(x + 1 + u, nx)
                number = d * nx + other

                @pl.when(k == 0)
                def _():
                    for copy in weight_copies(number):
                        copy.wait()
                source = field[p]
                value = (jnp.dot(weights[0, number], source, preferred_element_type=jnp.float32)
                         + jnp.dot(weights[1, number], source, preferred_element_type=jnp.float32))
                if u < nx - 1:
                    tx_a[d, other] = value[:half].astype(jnp.bfloat16)
                    cross_a(p, d, other, x).start()
                else:
                    part_a[d] = value[:half]

                @pl.when(d == z)
                def _():
                    part_b[other] = value[half:]

                @pl.when(d != z)
                def _():
                    tx_b[d, other] = value[half:].astype(jnp.bfloat16)

            @pl.when(d != z)
            def _():
                line_b(p, d, z).start()
            return inner

        lax.fori_loop(0, nz, multiply, 0)

        def collect_a(d):
            for other in others:
                cross_a(p, d, other, other).wait_recv()
                part_a[d] += rx_a[p, d, other].astype(jnp.float32)

        def pass_on(t, inner):
            d, way, neighbour, first = visit(t)

            @pl.when(d != z)
            def _():
                collect_a(d)
                for q in range(PIECES):
                    rows = pl.ds(q * quarter, quarter)

                    @pl.when(jnp.logical_not(first))
                    def _():
                        line_a(p, way, d, q, neighbour).wait_recv()
                        part_a[d, rows] += zr_a[p, way, d, rows]
                    line_a(p, way, d, q, neighbour).start()
            return inner

        early = (nz + 1) // 2
        lax.fori_loop(0, early, pass_on, 0)
        for level in levels:
            line_b(p, level, level).wait_recv()
            part_b[...] += zr_b[p, level].astype(jnp.float32)
        for other in others:
            cross_b(p, other, x).start()
        lax.fori_loop(early, nz, pass_on, 0)

        alpha = jnp.where(k == 0, 1.0, 2.0).astype(jnp.float32)
        beta = jnp.where(k == 0, 0.0, 1.0).astype(jnp.float32)
        weight = coef_ref[k + 1]

        def finish(part, summed):
            span = slice(part * half, (part + 1) * half)
            now = cur[span]
            moved = (1.0 - SHIFT) * now - inv_ref[span] * summed
            following = alpha * moved - beta * prev[span]

            @pl.when(k < ORDER - 1)
            def _():
                share(1 - p, part, inv_ref[span] * following)
            prev[span] = now
            cur[span] = following
            out_ref[span] = out_ref[span] + weight * following

        summed = part_b[x]
        for other in others:
            cross_b(p, other, other).wait_recv()
            summed = summed + rx_b[p, other]
        finish(1, summed)
        collect_a(z)
        for way, there in ((0, z > 0), (1, z < nz - 1)):
            @pl.when(there)
            def _():
                for q in range(PIECES):
                    rows = pl.ds(q * quarter, quarter)
                    line_a(p, way, z, q, z).wait_recv()
                    part_a[z, rows] += zr_a[p, way, z, rows]
        finish(0, part_a[z])

        for other in others:
            cross_b(p, other, x).wait_send()

        def drain(t, inner):
            d, way, neighbour, first = visit(t)
            for other in others:
                cross_a(p, d, other, x).wait_send()

            @pl.when(d != z)
            def _():
                line_b(p, d, z).wait_send()
                for q in range(PIECES):
                    line_a(p, way, d, q, neighbour).wait_send()
            return inner

        lax.fori_loop(0, nz, drain, 0)
        return carry

    lax.fori_loop(0, ORDER, step, 0)


def grid_of(n):
    nx = 1
    while nx * nx * 4 <= n and n % (nx * 2) == 0:
        nx *= 2
    return n // nx, nx


def solution(mesh):
    n_row, n_col = mesh.shape["row"], mesh.shape["col"]
    nz, nx = grid_of(n_row)

    def per_device(embedding, degrees, tile_values, tile_layout, tile_count, coefficients):
        tiles = tile_values[0, 0]
        block = tiles.shape[1]
        piece, width = embedding.shape
        half = piece // 2
        inv = lax.rsqrt(degrees.astype(jnp.float32))[:, None]
        inv = jnp.broadcast_to(inv, (piece, width))
        smem = pl.BlockSpec(memory_space=pltpu.SMEM)
        vmem = pl.BlockSpec(memory_space=pltpu.VMEM)
        anywhere = pl.BlockSpec(memory_space=pl.ANY)
        weight = jax.ShapeDtypeStruct((n_row, block, n_col * block), jnp.bfloat16)
        high, low = pl.pallas_call(
            functools.partial(merge_kernel, n_row, n_col),
            out_shape=(weight, weight),
            in_specs=[smem, smem, anywhere],
            out_specs=(anywhere, anywhere),
            scratch_shapes=[
                pltpu.VMEM((n_row * n_col, block, block), jnp.float32),
                pltpu.VMEM((DEPTH, CHUNK, block, block), jnp.bfloat16),
                pltpu.VMEM((2, 2, block, n_col * block), jnp.bfloat16),
                pltpu.SemaphoreType.DMA((DEPTH,)),
                pltpu.SemaphoreType.DMA((2, 2)),
            ],
            compiler_params=pltpu.CompilerParams(vmem_limit_bytes=VMEM_LIMIT),
        )(tile_count.reshape(1), tile_layout.reshape(-1), tiles)
        dma = pltpu.SemaphoreType.DMA
        f32 = jnp.float32
        return pl.pallas_call(
            functools.partial(filter_kernel, nz, nx, n_col),
            out_shape=jax.ShapeDtypeStruct((piece, width), f32),
            in_specs=[smem, vmem, vmem, anywhere, anywhere],
            out_specs=vmem,
            scratch_shapes=[
                pltpu.VMEM((2, n_row, block, n_col * block), jnp.bfloat16),
                pltpu.VMEM((piece, width), f32),
                pltpu.VMEM((piece, width), f32),
                pltpu.VMEM((2, n_col * piece, width), jnp.bfloat16),
                pltpu.VMEM((nz, half, width), f32),
                pltpu.VMEM((nx, half, width), f32),
                pltpu.VMEM((nz, nx, half, width), jnp.bfloat16),
                pltpu.VMEM((nz, nx, half, width), jnp.bfloat16),
                pltpu.VMEM((2, nz, nx, half, width), jnp.bfloat16),
                pltpu.VMEM((2, nx, half, width), f32),
                pltpu.VMEM((2, 2, nz, half, width), f32),
                pltpu.VMEM((2, nz, nx, half, width), jnp.bfloat16),
                dma((2, n_row)), dma((2, n_col)), dma((2, 2, n_col)),
                dma((nz, nx)), dma((2, nz, nx)),
                dma((nz, PIECES)), dma((2, 2, nz, PIECES)),
                dma((nz,)), dma((2, nz)),
                dma((nx,)), dma((2, nx)),
            ],
            compiler_params=pltpu.CompilerParams(
                collective_id=0, has_side_effects=True, vmem_limit_bytes=VMEM_LIMIT),
        )(coefficients, embedding, inv, high, low)

    return jax.shard_map(
        per_device, mesh=mesh,
        in_specs=(P(("row", "col"), None), P(("row", "col")),
                  P("row", "col", None, None, None), P("row", "col", None, None),
                  P("row", "col"), P()),
        out_specs=P(("row", "col"), None), check_vma=False)
```

```python
import functools

import jax
import jax.numpy as jnp
from jax import lax
from jax.experimental import pallas as pl
from jax.experimental.pallas import tpu as pltpu
from jax.sharding import PartitionSpec as P

ORDER = 6
SHIFT = 0.5
CHUNK = 4
DEPTH = 8
PIECES = 2
MESH = pl.DeviceIdType.MESH
VMEM_LIMIT = 60 * 1024 * 1024


def merge_kernel(n_row, n_col, count_ref, place_ref, tiles_ref, hi_ref, lo_ref,
                 total, landed, stage, in_sem, out_sem):
    block = tiles_ref.shape[1]
    count = count_ref[0]
    chunks = (count + CHUNK - 1) // CHUNK

    def fetch(chunk):
        slot = lax.rem(chunk, DEPTH)
        return pltpu.make_async_copy(
            tiles_ref.at[pl.ds(chunk * CHUNK, CHUNK)], landed.at[slot], in_sem.at[slot])

    for ahead in range(DEPTH):
        @pl.when(ahead < chunks)
        def _():
            fetch(jnp.int32(ahead)).start()

    def clear(place, carry):
        total[place] = jnp.zeros((block, block), jnp.float32)
        return carry

    lax.fori_loop(0, n_row * n_col, clear, 0)

    def add_chunk(chunk, carry):
        slot = lax.rem(chunk, DEPTH)
        fetch(chunk).wait()
        for inner in range(CHUNK):
            number = chunk * CHUNK + inner

            @pl.when(number < count)
            def _():
                place = place_ref[number]
                total[place] += landed[slot, inner].astype(jnp.float32)

        @pl.when(chunk + DEPTH < chunks)
        def _():
            fetch(chunk + DEPTH).start()
        return carry

    lax.fori_loop(0, chunks, add_chunk, 0)

    def outgoing(row):
        slot = lax.rem(row, 2)
        return (pltpu.make_async_copy(stage.at[slot, 0], hi_ref.at[row], out_sem.at[slot, 0]),
                pltpu.make_async_copy(stage.at[slot, 1], lo_ref.at[row], out_sem.at[slot, 1]))

    def put_row(row, carry):
        slot = lax.rem(row, 2)

        @pl.when(row >= 2)
        def _():
            for copy in outgoing(row - 2):
                copy.wait()
        for col in range(n_col):
            value = total[row * n_col + col]
            high = value.astype(jnp.bfloat16)
            stage[slot, 0, :, col * block:(col + 1) * block] = high
            stage[slot, 1, :, col * block:(col + 1) * block] = (
                value - high.astype(jnp.float32)).astype(jnp.bfloat16)
        for copy in outgoing(row):
            copy.start()
        return carry

    lax.fori_loop(0, n_row, put_row, 0)
    for row in (n_row - 2, n_row - 1):
        for copy in outgoing(jnp.int32(row)):
            copy.wait()


def filter_kernel(nz, nx, nc, coef_ref, emb_ref, inv_ref, hi_ref, lo_ref, out_ref,
                  weights, prev, cur, field, part_a, part_b, tx_a, tx_b, rx_a, rx_b, zr_a, zr_b,
                  w_sem, ag_send, ag_recv, xa_send, xa_recv, za_send, za_recv,
                  zb_send, zb_recv, xb_send, xb_recv):
    r = lax.axis_index("row")
    c = lax.axis_index("col")
    z, x = r // nx, lax.rem(r, nx)
    piece = emb_ref.shape[0]
    half = piece // 2
    quarter = half // PIECES

    def rows_of(owner, part):
        return pl.ds(pl.multiple_of(owner * piece + part * half, half), half)

    def remote(src, dst, send_sem, recv_sem, **where):
        return pltpu.make_async_remote_copy(
            src_ref=src, dst_ref=dst, send_sem=send_sem, recv_sem=recv_sem,
            device_id={"row": where.get("row", r), "col": where.get("col", c)},
            device_id_type=MESH)

    def gather_copy(p, part, offset, owner):
        spot = field.at[p, rows_of(owner, part)]
        return remote(spot, spot, ag_send.at[part, offset], ag_recv.at[p, part, owner],
                      col=lax.rem(c + offset, nc))

    def cross_a(p, d, other, source):
        return remote(tx_a.at[d, other], rx_a.at[p, d, source],
                      xa_send.at[d, other], xa_recv.at[p, d, source], row=z * nx + other)

    def cross_b(p, other, source):
        return remote(part_b.at[other], rx_b.at[p, source],
                      xb_send.at[other], xb_recv.at[p, source], row=z * nx + other)

    def line_a(p, way, d, q, neighbour):
        rows = pl.ds(q * quarter, quarter)
        return remote(part_a.at[d, rows], zr_a.at[p, way, d, rows],
                      za_send.at[d, q], za_recv.at[p, way, d, q], row=neighbour * nx + x)

    def line_b(p, d, source):
        return remote(tx_b.at[d], zr_b.at[p, source],
                      zb_send.at[d], zb_recv.at[p, source], row=d * nx + x)

    def weight_copies(number):
        return (pltpu.make_async_copy(hi_ref.at[number], weights.at[0, number], w_sem.at[0, number]),
                pltpu.make_async_copy(lo_ref.at[number], weights.at[1, number], w_sem.at[1, number]))

    def visit(t):
        d = jnp.where(2 * z >= nz, t, nz - 1 - t)
        upward = d > z
        way = jnp.where(upward, 0, 1)
        neighbour = jnp.clip(jnp.where(upward, z + 1, z - 1), 0, nz - 1)
        first = jnp.where(upward, z == 0, z == nz - 1)
        return d, way, neighbour, first

    others = [lax.rem(x + 1 + u, nx) for u in range(nx - 1)]
    levels = [lax.rem(z + 1 + u, nz) for u in range(nz - 1)]

    def share(p, part, value):
        field[p, rows_of(c, part)] = value.astype(jnp.bfloat16)
        for offset in range(1, nc):
            gather_copy(p, part, offset, c).start()

    def load(t, carry):
        d = visit(t)[0]
        for u in range(nx):
            for copy in weight_copies(d * nx + lax.rem(x + 1 + u, nx)):
                copy.start()
        return carry

    barrier = pltpu.get_barrier_semaphore()
    for other in others:
        pl.semaphore_signal(barrier, inc=1, device_id={"row": z * nx + other, "col": c},
                            device_id_type=MESH)
    for level in levels:
        pl.semaphore_signal(barrier, inc=1, device_id={"row": level * nx + x, "col": c},
                            device_id_type=MESH)
    for offset in range(1, nc):
        pl.semaphore_signal(barrier, inc=1, device_id={"row": r, "col": lax.rem(c + offset, nc)},
                            device_id_type=MESH)
    lax.fori_loop(0, nz, load, 0)
    start = emb_ref[...]
    prev[...] = start
    cur[...] = start
    out_ref[...] = coef_ref[0] * start
    pl.semaphore_wait(barrier, nx - 1 + nz - 1 + nc - 1)
    for part in range(2):
        span = slice(part * half, (part + 1) * half)
        share(0, part, inv_ref[span] * emb_ref[span])

    def step(k, carry):
        p = lax.rem(k, 2)
        for offset in range(1, nc):
            for part in range(2):
                copy = gather_copy(p, part, offset, lax.rem(c + offset, nc))
                copy.wait_send()
                copy.wait_recv()

        def multiply(t, inner):
            d = visit(t)[0]
            for u in range(nx):
                other = lax.rem(x + 1 + u, nx)
                number = d * nx + other

                @pl.when(k == 0)
                def _():
                    for copy in weight_copies(number):
                        copy.wait()
                source = field[p]
                value = (jnp.dot(weights[0, number], source, preferred_element_type=jnp.float32)
                         + jnp.dot(weights[1, number], source, preferred_element_type=jnp.float32))
                if u < nx - 1:
                    tx_a[d, other] = value[:half]
                    cross_a(p, d, other, x).start()
                else:
                    part_a[d] = value[:half]

                @pl.when(d == z)
                def _():
                    part_b[other] = value[half:]

                @pl.when(d != z)
                def _():
                    tx_b[d, other] = value[half:].astype(jnp.bfloat16)

            @pl.when(d != z)
            def _():
                line_b(p, d, z).start()
            return inner

        lax.fori_loop(0, nz, multiply, 0)

        def collect_a(d):
            for other in others:
                cross_a(p, d, other, other).wait_recv()
                part_a[d] += rx_a[p, d, other]

        def pass_on(t, inner):
            d, way, neighbour, first = visit(t)

            @pl.when(d != z)
            def _():
                collect_a(d)
                for q in range(PIECES):
                    rows = pl.ds(q * quarter, quarter)

                    @pl.when(jnp.logical_not(first))
                    def _():
                        line_a(p, way, d, q, neighbour).wait_recv()
                        part_a[d, rows] += zr_a[p, way, d, rows]
                    line_a(p, way, d, q, neighbour).start()
            return inner

        early = (nz + 1) // 2
        lax.fori_loop(0, early, pass_on, 0)
        for level in levels:
            line_b(p, level, level).wait_recv()
            part_b[...] += zr_b[p, level].astype(jnp.float32)
        for other in others:
            cross_b(p, other, x).start()
        lax.fori_loop(early, nz, pass_on, 0)

        alpha = jnp.where(k == 0, 1.0, 2.0).astype(jnp.float32)
        beta = jnp.where(k == 0, 0.0, 1.0).astype(jnp.float32)
        weight = coef_ref[k + 1]

        def finish(part, summed):
            span = slice(part * half, (part + 1) * half)
            now = cur[span]
            moved = (1.0 - SHIFT) * now - inv_ref[span] * summed
            following = alpha * moved - beta * prev[span]

            @pl.when(k < ORDER - 1)
            def _():
                share(1 - p, part, inv_ref[span] * following)
            prev[span] = now
            cur[span] = following
            out_ref[span] = out_ref[span] + weight * following

        summed = part_b[x]
        for other in others:
            cross_b(p, other, other).wait_recv()
            summed = summed + rx_b[p, other]
        finish(1, summed)
        collect_a(z)
        for way, there in ((0, z > 0), (1, z < nz - 1)):
            @pl.when(there)
            def _():
                for q in range(PIECES):
                    rows = pl.ds(q * quarter, quarter)
                    line_a(p, way, z, q, z).wait_recv()
                    part_a[z, rows] += zr_a[p, way, z, rows]
        finish(0, part_a[z])

        for other in others:
            cross_b(p, other, x).wait_send()

        def drain(t, inner):
            d, way, neighbour, first = visit(t)
            for other in others:
                cross_a(p, d, other, x).wait_send()

            @pl.when(d != z)
            def _():
                line_b(p, d, z).wait_send()
                for q in range(PIECES):
                    line_a(p, way, d, q, neighbour).wait_send()
            return inner

        lax.fori_loop(0, nz, drain, 0)
        return carry

    lax.fori_loop(0, ORDER, step, 0)


def grid_of(n):
    nx = 1
    while nx * nx * 4 <= n and n % (nx * 2) == 0:
        nx *= 2
    return n // nx, nx


def solution(mesh):
    n_row, n_col = mesh.shape["row"], mesh.shape["col"]
    nz, nx = grid_of(n_row)

    def per_device(embedding, degrees, tile_values, tile_layout, tile_count, coefficients):
        tiles = tile_values[0, 0]
        block = tiles.shape[1]
        piece, width = embedding.shape
        half = piece // 2
        wide = jnp.broadcast_to(degrees[:, None], (piece, width))
        inv = lax.rsqrt(wide.astype(jnp.float32))
        layout = tile_layout[0, 0]
        places = layout[:, 0] * n_col + layout[:, 1]
        smem = pl.BlockSpec(memory_space=pltpu.SMEM)
        vmem = pl.BlockSpec(memory_space=pltpu.VMEM)
        anywhere = pl.BlockSpec(memory_space=pl.ANY)
        weight = jax.ShapeDtypeStruct((n_row, block, n_col * block), jnp.bfloat16)
        high, low = pl.pallas_call(
            functools.partial(merge_kernel, n_row, n_col),
            out_shape=(weight, weight),
            in_specs=[smem, smem, anywhere],
            out_specs=(anywhere, anywhere),
            scratch_shapes=[
                pltpu.VMEM((n_row * n_col, block, block), jnp.float32),
                pltpu.VMEM((DEPTH, CHUNK, block, block), jnp.bfloat16),
                pltpu.VMEM((2, 2, block, n_col * block), jnp.bfloat16),
                pltpu.SemaphoreType.DMA((DEPTH,)),
                pltpu.SemaphoreType.DMA((2, 2)),
            ],
            compiler_params=pltpu.CompilerParams(vmem_limit_bytes=VMEM_LIMIT),
        )(tile_count.reshape(1), places, tiles)
        dma = pltpu.SemaphoreType.DMA
        f32 = jnp.float32
        return pl.pallas_call(
            functools.partial(filter_kernel, nz, nx, n_col),
            out_shape=jax.ShapeDtypeStruct((piece, width), f32),
            in_specs=[smem, vmem, vmem, anywhere, anywhere],
            out_specs=vmem,
            scratch_shapes=[
                pltpu.VMEM((2, n_row, block, n_col * block), jnp.bfloat16),
                pltpu.VMEM((piece, width), f32),
                pltpu.VMEM((piece, width), f32),
                pltpu.VMEM((2, n_col * piece, width), jnp.bfloat16),
                pltpu.VMEM((nz, half, width), f32),
                pltpu.VMEM((nx, half, width), f32),
                pltpu.VMEM((nz, nx, half, width), f32),
                pltpu.VMEM((nz, nx, half, width), jnp.bfloat16),
                pltpu.VMEM((2, nz, nx, half, width), f32),
                pltpu.VMEM((2, nx, half, width), f32),
                pltpu.VMEM((2, 2, nz, half, width), f32),
                pltpu.VMEM((2, nz, nx, half, width), jnp.bfloat16),
                dma((2, n_row)), dma((2, n_col)), dma((2, 2, n_col)),
                dma((nz, nx)), dma((2, nz, nx)),
                dma((nz, PIECES)), dma((2, 2, nz, PIECES)),
                dma((nz,)), dma((2, nz)),
                dma((nx,)), dma((2, nx)),
            ],
            compiler_params=pltpu.CompilerParams(
                collective_id=0, has_side_effects=True, vmem_limit_bytes=VMEM_LIMIT),
        )(coefficients, embedding, inv, high, low)

    return jax.shard_map(
        per_device, mesh=mesh,
        in_specs=(P(("row", "col"), None), P(("row", "col")),
                  P("row", "col", None, None, None), P("row", "col", None, None),
                  P("row", "col"), P()),
        out_specs=P(("row", "col"), None), check_vma=False)
```
